512 devices in a mesh: dp: 8 (over z), fsdp: 64 (over y, x, core).
Axes of the slice: x: 4, y: 8, z: 8, core: 2. Of those that a mesh axis runs over, the one named last changes fastest.
Arguments:
- small_cols: bfloat16 [393216, 128], P(('dp', 'fsdp')), may hold values from -24 to 24
- wide_cols: bfloat16 [393216, 2, 1536], P(('dp', 'fsdp')), may hold values from -24 to 24
- token_counts: int32 [512], P(('dp', 'fsdp')), may hold values from 144 to 768, as said below
- loss_sums: float32 [512], P(('dp', 'fsdp'))
- weight: float32 [128, 1536], P('fsdp'), may hold values from -0.75 to 0.75
- first_moment: float32 [128, 1536], P('fsdp'), may hold values from -0.002 to 0.002
- second_moment: float32 [128, 1536], P('fsdp'), may hold values from 1e-07 to 1e-06
- step: int32 [], replicated, may hold values from 1 to 2999
Outputs:
- new_weight: float32 [128, 1536], P('fsdp')
- new_first: float32 [128, 1536], P('fsdp')
- new_second: float32 [128, 1536], P('fsdp')
- adam_step: float32 [128, 1536], P('fsdp')
- grad_norm: float32 [], replicated
- mean_loss: float32 [], replicated
The draws below stay inside these ranges and needn't reach their ends.
Inputs may be any that keep to these rules, and one draw needn't show every extreme that they name: `token_counts`: each count is f * h * w with f from 1 to 3 and h, w from 12 to 16; in every draw some device's count is exactly 768.
All inputs are finite; a program needn't handle non-finite values.
Results may differ from the reference program's by a relative error of at most 0.0003.
Values sent between devices are 32-bit elements; how exact they have to be, the bound alone decides.
A program may use at most 64 MiB of HBM per device.

```python
import math
import jax
import jax.numpy as jnp
from jax import lax

D = 1536
PATCH = 64
FRAMES = 3
GRID = 16
CAP = 768
ROWS = 128
DEVS = 512


def draw_token_counts(key, part):
    keys = jax.random.split(jax.random.fold_in(key, 11), 4)
    frames = jax.random.randint(keys[0], (DEVS,), 1, FRAMES + 1)
    heights = jax.random.randint(keys[1], (DEVS,), 3 * GRID // 4, GRID + 1)
    widths = jax.random.randint(keys[2], (DEVS,), 3 * GRID // 4, GRID + 1)
    chosen = jax.random.randint(keys[3], (), 0, DEVS)
    counts = frames * heights * widths
    fullest = jnp.full((DEVS,), FRAMES * GRID * GRID, jnp.int32)
    return jnp.where(jnp.arange(DEVS) == chosen, fullest, counts).astype(jnp.int32)


def draw_loss_sums(key, part):
    keys = jax.random.split(jax.random.fold_in(key, 23), 1)
    ramp = 1.0 + 2.0 * jnp.arange(DEVS, dtype=jnp.float32) / max(DEVS - 1, 1)
    spread = jax.random.uniform(keys[0], (DEVS,), jnp.float32, 0.5, 1.5)
    values = 300.0 * ramp * spread
    return jnp.maximum(values, 10.0).astype(jnp.float32)


def with_spikes(drawn, own_key, source, target, parts, factor):
    def block_of(position):
        return (jnp.arange(drawn.shape[position]) // (drawn.shape[position] // parts)).reshape((-1,) + (1,) * (drawn.ndim - 1 - position))

    near = jax.random.permutation(own_key, parts)[block_of(target)]
    other_side = (block_of(target) + parts // 2) % parts
    return jnp.where((block_of(source) == near) | (block_of(source) == other_side), factor * drawn, drawn)


def steps_of(stream_key, shape, cuts, low, top_value):
    factor_of, own = 1.0, jax.random.fold_in(stream_key, 6)
    for axis_at, parts in cuts:
        steps = jnp.exp(jax.random.uniform(jax.random.fold_in(own, axis_at), (parts,), jnp.float32, low / len(cuts), top_value / len(cuts)))
        factor_of = factor_of * jnp.repeat(steps, shape[axis_at] // parts).reshape([-1 if axis == axis_at else 1 for axis in range(len(shape))])
    return factor_of


def gaussian(rng, dims, width, bound, cuts=(), held_as=jnp.bfloat16):
    drawn = width * jax.random.normal(rng, dims, jnp.float32)
    if cuts:
        drawn = drawn * steps_of(rng, dims, cuts, -0.22, 0.18)
    return jnp.clip(drawn, -bound, bound).astype(held_as)


def bell_draw_with(stream_key, extent, deviation, limit, cuts, heavy, kind=jnp.bfloat16):
    result = deviation * jax.random.normal(stream_key, extent, jnp.float32)
    if cuts:
        result = result * steps_of(stream_key, extent, cuts, -0.22, 0.18)
    return jnp.clip(with_spikes(result, jax.random.fold_in(stream_key, 3), *heavy), -limit, limit).astype(kind)


def setup_inputs(seed: int = 0) -> dict:
    splits = jax.random.split(jax.random.key(seed), 9)
    return {
        "small_cols": bell_draw_with(splits[0], (DEVS * CAP, ROWS), 1.0, 24.0, ((0, 512),), (0, 1, 128, 5.5)),
        "wide_cols": gaussian(splits[1], (DEVS * CAP, 2, D), 4.0, 24.0, ((0, 512),)),
        "token_counts": draw_token_counts(jax.random.fold_in(splits[8], 71), 0),
        "loss_sums": draw_loss_sums(jax.random.fold_in(splits[8], 71), 0),
        "weight": gaussian(splits[4], (ROWS, D), PATCH ** -0.5, 0.75, ((0, 64),), jnp.float32),
        "first_moment": gaussian(splits[5], (ROWS, D), 0.0003, 0.002, ((0, 64),), jnp.float32),
        "second_moment": jnp.clip(jnp.exp(math.log(9.999999974752427e-07) - 2.3025851 * jax.random.uniform(splits[6], (ROWS, D), jnp.float32) ** steps_of(splits[6], (ROWS, D), ((0, 64),), -0.2, 0.2)), 1.0000000116860974e-07, 9.999999974752427e-07),
        "step": jax.random.randint(splits[7], (), 1, 3000).astype(jnp.int32),
    }


MAX_NORM = 1.0
BETA_FIRST = 0.9
BETA_SECOND = 0.999
EPSILON_ADAM = 1e-08
LEARN_RATE = 0.02
DECAY_RATE = 0.1

def reference(small_cols, wide_cols, token_counts, loss_sums, weight, first_moment, second_moment, step):
    positions = jnp.arange(CAP, dtype=jnp.int32)

    def add_device(running, device):
        offset = (device * CAP).astype(jnp.int32)
        narrow = lax.dynamic_slice_in_dim(small_cols, offset, CAP, 0).astype(jnp.float32)
        broad = lax.dynamic_slice_in_dim(wide_cols, offset, CAP, 0).astype(jnp.float32)
        is_live = positions < token_counts[device]
        narrow = jnp.where(is_live[:, None], narrow, jnp.zeros_like(narrow))
        portion = jnp.einsum('thc,thd->hcd', narrow.reshape(CAP, 2, PATCH), broad)
        return (running + portion.reshape(ROWS, D), None)
    raw_sum, unused = lax.scan(add_device, jnp.zeros((ROWS, D), jnp.float32), jnp.arange(DEVS, dtype=jnp.int32))
    token_total = jnp.sum(token_counts.astype(jnp.float32))
    loss_total = jnp.sum(loss_sums)
    gradient = raw_sum / token_total
    grad_norm = jnp.sqrt(jnp.sum(gradient * gradient))
    mean_loss = loss_total / token_total
    clip_factor = jnp.minimum(1.0, MAX_NORM / (grad_norm + 1e-06))
    clipped = gradient * clip_factor
    new_first = BETA_FIRST * first_moment + (1.0 - BETA_FIRST) * clipped
    new_second = BETA_SECOND * second_moment + (1.0 - BETA_SECOND) * clipped * clipped
    step_float = step.astype(jnp.float32)
    first_hat = new_first / (1.0 - jnp.power(jnp.float32(BETA_FIRST), step_float))
    second_hat = new_second / (1.0 - jnp.power(jnp.float32(BETA_SECOND), step_float))
    adam_step = first_hat / (jnp.sqrt(second_hat) + EPSILON_ADAM) + DECAY_RATE * weight
    new_weight = weight - LEARN_RATE * adam_step
    return (new_weight, new_first, new_second, adam_step, grad_norm, mean_loss)
```

```python
import functools
import math

import jax
import jax.numpy as jnp
import numpy as np
from jax import lax
from jax.experimental import pallas as pl
from jax.experimental.pallas import tpu as pltpu
from jax.sharding import PartitionSpec as P

MAX_NORM = 1.0
BETA_FIRST = 0.9
BETA_SECOND = 0.999
EPSILON_ADAM = 1e-08
LEARN_RATE = 0.02
DECAY_RATE = 0.1

MESH = pl.DeviceIdType.MESH
F32 = jnp.float32
BF16 = jnp.bfloat16
TOKENS, ROWS, WIDTH = 768, 128, 1536
TILES = WIDTH // 128
CHUNKS = 6
GROUPS = 3
X, Y, Z = 4, 8, 8
PLANE = 64


def iota(shape, dim):
    return lax.broadcasted_iota(jnp.int32, shape, dim)


def one_minus_power(beta, step):
    u = step * F32(math.log(float(np.float32(beta))))
    series = jnp.ones_like(u)
    for n in range(10, 1, -1):
        series = 1.0 + u * series * F32(1.0 / n)
    return jnp.where(u > -0.5, -u * series, 1.0 - jnp.exp(u))


def left_operand(small, count, left):
    row, col = iota((128, 128), 0), iota((128, 128), 1)
    core, x, r, y = row >> 6, (row >> 4) & 3, (row >> 3) & 1, row & 7
    order = (col == y * 16 + x * 4 + core * 2 + r).astype(F32).astype(BF16)
    second = y >= 4
    spread_row, spread_col = iota((256, 256), 0), iota((256, 256), 1)
    spread = (spread_col == ((spread_row & 127) << 1) + (spread_row >> 7)).astype(F32).astype(BF16)
    for b in range(TOKENS // 128):
        block = small[pl.ds(b * 128, 128), :].astype(F32)
        block = jnp.where(row + b * 128 < count, block, 0.0).astype(BF16)
        turned = lax.dot_general(order, block, (((1,), (1,)), ((), ())), preferred_element_type=F32)
        halves = jnp.concatenate(
            [jnp.where(second, 0.0, turned), jnp.where(second, turned, 0.0)], axis=1
        ).astype(BF16)
        left[:, pl.ds(b * 256, 256)] = jnp.dot(halves, spread, preferred_element_type=F32).astype(BF16)


def kernel(
    small_hbm, wide_hbm, count_hbm, loss_hbm, weight_hbm, first_hbm, second_hbm, step_hbm,
    new_weight, new_first, new_second, adam, scalars,
    small, wide, left, part, core_in, held, opposite_in, direct_in, merged, merged_in, lines, y_in, y_sum,
    z_in, pair, pair_in, note, notes_in, states, count_smem, loss_smem, step_smem,
    load_sem, wide_sem, smem_sem, core_send, core_recv, opp_send, opp_recv, dir_send, dir_recv, mer_send, mer_recv,
    y_send, y_recv, z_send, z_recv, pair_send, pair_recv, note_send, note_recv, relay,
):
    z, f = lax.axis_index("dp"), lax.axis_index("fsdp")
    c, x, y = lax.rem(f, 2), lax.rem(lax.div(f, 2), X), lax.div(f, 2 * X)

    def at(z_, y_, x_, c_):
        return (z_, (y_ * X + x_) * 2 + c_)

    x_up, x_down, x_far = lax.rem(x + 1, X), lax.rem(x + X - 1, X), lax.rem(x + 2, X)
    y_up, y_down = lax.rem(y + 1, Y), lax.rem(y + Y - 1, Y)
    z_up, z_down = lax.rem(z + 1, Z), lax.rem(z + Z - 1, Z)
    partner = at(z, y, x, 1 - c)
    to_x_up, to_x_down = at(z, y, x_up, c), at(z, y, x_down, c)
    ring = (at(z, y_up, x, c), at(z, y_down, x, c), at(z_up, y, x, c), at(z_down, y, x, c))

    barrier = pltpu.get_barrier_semaphore()
    for device in (partner, to_x_up, to_x_down) + ring:
        pl.semaphore_signal(barrier, inc=1, device_id=device, device_id_type=MESH)

    loads = [pltpu.make_async_copy(small_hbm, small, load_sem.at[0])]
    smem_loads = [
        pltpu.make_async_copy(count_hbm, count_smem, smem_sem.at[0]),
        pltpu.make_async_copy(loss_hbm, loss_smem, smem_sem.at[1]),
        pltpu.make_async_copy(step_hbm, step_smem, smem_sem.at[2]),
    ]
    columns = [
        pltpu.make_async_copy(wide_hbm.at[:, :, pl.ds(t * 128, 128)], wide.at[t], wide_sem.at[t])
        for t in range(TILES)
    ]
    for n, array in enumerate((weight_hbm, first_hbm, second_hbm)):
        loads.append(pltpu.make_async_copy(array, states.at[n], load_sem.at[n + 1]))
    for copy in loads[:1] + smem_loads + columns + loads[1:]:
        copy.start()

    def remote(src, dst, send, recv, device):
        copy = pltpu.make_async_remote_copy(
            src_ref=src, dst_ref=dst, send_sem=send, recv_sem=recv, device_id=device, device_id_type=MESH
        )
        copy.start()
        return copy

    def wait_bytes(ref, sem):
        pltpu.make_async_copy(ref, ref, sem).wait()

    def relay_signal(n):
        for device in ring:
            pl.semaphore_signal(relay.at[n], inc=1, device_id=device, device_id_type=MESH)

    for copy in smem_loads[:2]:
        copy.wait()
    loads[0].wait()
    left_operand(small, count_smem[0], left)

    to_core, to_opp, to_dir, to_mer = {}, {}, {}, {}

    def multiply(k):
        columns[2 * k].wait()
        columns[2 * k + 1].wait()
        right = jnp.concatenate([wide[2 * k + n].reshape(2 * TOKENS, 128) for n in range(2)], axis=1)
        product = jnp.dot(left[...], right, preferred_element_type=F32)
        part[k] = product.reshape(2, X, 16, 256)

    def core_out(k):
        to_core[k] = remote(part.at[k, 1 - c], core_in.at[k], core_send.at[k], core_recv.at[k], partner)

    def core_add(k):
        to_core[k].wait_recv()
        held[k] = part[k, c] + core_in[k]
        near, far = (to_x_up, to_x_down) if k % 2 == 0 else (to_x_down, to_x_up)
        to_opp[k] = remote(held.at[k, x_far], opposite_in.at[k], opp_send.at[k], opp_recv.at[k], near)
        other = x_down if k % 2 == 0 else x_up
        to_dir[k] = remote(held.at[k, other], direct_in.at[k], dir_send.at[k], dir_recv.at[k], far)

    def x_merge(k):
        to_opp[k].wait_recv()
        near, index = (to_x_up, x_up) if k % 2 == 0 else (to_x_down, x_down)
        merged[k] = held[k, index] + opposite_in[k]
        to_mer[k] = remote(merged.at[k], merged_in.at[k], mer_send.at[k], mer_recv.at[k], near)

    def x_final(k):
        to_dir[k].wait_recv()
        to_mer[k].wait_recv()
        total = held[k, x] + direct_in[k] + merged_in[k]
        g, half = k // 2, k % 2
        for r in range(2):
            for t in range(2):
                lines[g, pl.ds(2 * (2 * half + t) + r, 8, stride=8), :] = total[8 * r : 8 * r + 8, 128 * t : 128 * t + 128]

    def y_out(g):
        for d in range(1, Y):
            to = lax.rem(y + d, Y)
            remote(
                lines.at[g, pl.ds(pl.multiple_of(to * 8, 8), 8)], y_in.at[g, d - 1],
                y_send.at[g], y_recv.at[g], at(z, to, x, c),
            )

    def y_add(g):
        wait_bytes(y_in.at[g], y_recv.at[g])
        total = lines[g, pl.ds(pl.multiple_of(y * 8, 8), 8), :]
        for d in range(Y - 1):
            total = total + y_in[g, d]
        y_sum[g] = total
        z_in[g, z] = total
        for d in range(1, Z):
            to = lax.rem(z + d, Z)
            remote(y_sum.at[g], z_in.at[g, z], z_send.at[g], z_recv.at[g], at(to, y, x, c))

    multiply(0)
    pl.semaphore_wait(barrier, 7)
    core_out(0)
    relay_signal(0)
    multiply(1)
    core_out(1)
    multiply(2)
    core_out(2)
    core_add(0)
    pl.semaphore_wait(relay.at[0], 4)
    relay_signal(1)
    multiply(3)
    core_out(3)
    core_add(1)
    multiply(4)
    core_out(4)
    core_add(2)
    pl.semaphore_wait(relay.at[1], 4)
    relay_signal(2)
    multiply(5)
    core_out(5)
    core_add(3)
    core_add(4)
    x_merge(0)
    core_add(5)
    x_merge(1)
    pl.semaphore_wait(relay.at[2], 4)

    lane = iota((1, 128), 1)
    mine = jnp.where(
        lane == 64, count_smem[0].astype(F32), jnp.where(lane == 65, loss_smem[0], 0.0)
    )
    pair[...] = mine
    pair_in[z] = mine
    for d in range(1, Z):
        remote(pair, pair_in.at[z], pair_send, pair_recv, at(lax.rem(z + d, Z), y, x, c))

    x_merge(2)
    x_final(0)
    x_merge(3)
    x_final(1)
    y_out(0)
    x_merge(4)
    x_final(2)
    x_merge(5)
    x_final(3)
    y_out(1)
    x_final(4)
    x_final(5)
    y_out(2)

    for g in range(GROUPS):
        y_add(g)
    totals = []
    squares = jnp.zeros((8, 128), F32)
    for g in range(GROUPS):
        wait_bytes(z_in.at[g, pl.ds(0, Z - 1)], z_recv.at[g])
        total = z_in[g, 0]
        for n in range(1, Z):
            total = total + z_in[g, n]
        totals.append(total)
        squares = squares + total * total
    wait_bytes(pair_in.at[pl.ds(0, Z - 1)], pair_recv)
    pairs = pair_in[0]
    for n in range(1, Z):
        pairs = pairs + pair_in[n]
    squares = jnp.sum(squares, axis=0, keepdims=True)
    squares = squares + pltpu.roll(squares, 64, 1)
    mine = jnp.where(lane < 64, squares, pairs)
    note[...] = mine
    notes_in[f] = mine
    for d in range(1, PLANE):
        to = lax.rem(f + d, PLANE)
        remote(note, notes_in.at[f], note_send, note_recv, (z, to))

    for copy in loads[1:] + smem_loads[2:]:
        copy.wait()
    step = jnp.full((8, 128), step_smem[0].astype(F32), F32)
    first_scale = 1.0 / one_minus_power(BETA_FIRST, step)
    second_scale = 1.0 / one_minus_power(BETA_SECOND, step)

    wait_bytes(notes_in.at[pl.ds(0, PLANE - 1)], note_recv)
    everything = jnp.sum(notes_in[...].reshape(PLANE, 128), axis=0, keepdims=True)
    square_total = jnp.sum(jnp.where(lane < 64, everything, 0.0), axis=1, keepdims=True)
    token_total = jnp.sum(jnp.where(lane == 64, everything, 0.0), axis=1, keepdims=True)
    loss_total = jnp.sum(jnp.where(lane == 65, everything, 0.0), axis=1, keepdims=True)
    grad_norm = jnp.sqrt(square_total) / token_total
    clip_factor = jnp.minimum(1.0, MAX_NORM / (grad_norm + 1e-06))
    scalars[...] = jnp.where(lane == 0, grad_norm, loss_total / token_total)
    kept = [states[n].reshape(GROUPS, 8, 128) for n in range(3)]
    for g in range(GROUPS):
        clipped = totals[g] / token_total * clip_factor
        weight, first, second = kept[0][g], kept[1][g], kept[2][g]
        first = BETA_FIRST * first + (1.0 - BETA_FIRST) * clipped
        second = BETA_SECOND * second + (1.0 - BETA_SECOND) * clipped * clipped
        update = (first * first_scale) / (jnp.sqrt(second * second_scale) + EPSILON_ADAM) + DECAY_RATE * weight
        new_first[g] = first
        new_second[g] = second
        adam[g] = update
        new_weight[g] = weight - LEARN_RATE * update

    for k in range(CHUNKS):
        for copies in (to_core, to_opp, to_dir, to_mer):
            copies[k].wait_send()
    for g in range(GROUPS):
        wait_bytes(y_in.at[g], y_send.at[g])
        wait_bytes(z_in.at[g, pl.ds(0, Z - 1)], z_send.at[g])
    wait_bytes(pair_in.at[pl.ds(0, Z - 1)], pair_send)
    wait_bytes(notes_in.at[pl.ds(0, PLANE - 1)], note_send)


def in_tiles(array):
    return array.reshape(2, TILES, 128).transpose(1, 0, 2)


def in_rows(array):
    return array.reshape(TILES, 2, 128).transpose(1, 0, 2).reshape(2, WIDTH)


def on_device(
    small_cols, wide_cols, token_counts, loss_sums, weight, first_moment, second_moment, step
):
    vmem, dma = pltpu.VMEM, pltpu.SemaphoreType.DMA
    block = jax.ShapeDtypeStruct((GROUPS, 8, 128), F32)
    *arrays, scalars = pl.pallas_call(
        kernel,
        name="reduce_and_step",
        out_shape=[block] * 4 + [jax.ShapeDtypeStruct((1, 128), F32)],
        in_specs=[pl.BlockSpec(memory_space=pl.ANY)] * 8,
        out_specs=[pl.BlockSpec(memory_space=pltpu.VMEM)] * 5,
        scratch_shapes=[
            vmem((TOKENS, ROWS), BF16),
            vmem((TILES, TOKENS, 2, 128), BF16),
            vmem((ROWS, 2 * TOKENS), BF16),
            vmem((CHUNKS, 2, X, 16, 256), F32),
            vmem((CHUNKS, X, 16, 256), F32),
            vmem((CHUNKS, X, 16, 256), F32),
            vmem((CHUNKS, 16, 256), F32),
            vmem((CHUNKS, 16, 256), F32),
            vmem((CHUNKS, 16, 256), F32),
            vmem((CHUNKS, 16, 256), F32),
            vmem((GROUPS, 8 * Y, 128), F32),
            vmem((GROUPS, Y - 1, 8, 128), F32),
            vmem((GROUPS, 8, 128), F32),
            vmem((GROUPS, Z, 8, 128), F32),
            vmem((1, 128), F32),
            vmem((Z, 1, 128), F32),
            vmem((1, 128), F32),
            vmem((PLANE, 1, 128), F32),
            vmem((3, TILES, 2, 128), F32),
            pltpu.SMEM((1,), jnp.int32),
            pltpu.SMEM((1,), F32),
            pltpu.SMEM((1,), jnp.int32),
            dma((4,)),
            dma((TILES,)),
            dma((3,)),
        ]
        + [dma((CHUNKS,))] * 8
        + [dma((GROUPS,))] * 4
        + [dma(())] * 4
        + [pltpu.SemaphoreType.REGULAR((3,))],
        compiler_params=pltpu.CompilerParams(
            collective_id=0, has_side_effects=True, vmem_limit_bytes=67_043_328
        ),
    )(
        small_cols, wide_cols, token_counts, loss_sums,
        in_tiles(weight), in_tiles(first_moment), in_tiles(second_moment), step.reshape(1),
    )
    new_weight, new_first, new_second, adam = (in_rows(a) for a in arrays)
    return (new_weight, new_first, new_second, adam, scalars[0, 0], scalars[0, 1])


def solution(mesh):
    in_specs = (
        P(("dp", "fsdp"), None),
        P(("dp", "fsdp"), None, None),
        P(("dp", "fsdp")),
        P(("dp", "fsdp")),
        P("fsdp", None),
        P("fsdp", None),
        P("fsdp", None),
        P(),
    )
    out_specs = (P("fsdp", None), P("fsdp", None), P("fsdp", None), P("fsdp", None), P(), P())
    return jax.shard_map(
        on_device, mesh=mesh, in_specs=in_specs, out_specs=out_specs, check_vma=False
    )
```
